8 devices in a mesh: side: 2 (over z, y), rep: 4 (over x, core).
Axes of the slice: x: 2, y: 2, z: 1, core: 2. Of those that a mesh axis runs over, the one named last changes fastest.
Arguments:
- w_up: float32 [2, 1, 1536, 8960], P('side', None, 'rep')
- w_down: float32 [2, 1, 8960, 1536], P('side', None, None, 'rep')
- g_up: float32 [2, 1, 1536, 8960], P('side', None, 'rep')
- g_down: float32 [2, 1, 8960, 1536], P('side', None, None, 'rep')
- learn_rate: float32 [1], replicated
- old_up: bfloat16 [2, 4, 1, 1536, 8960], P('side', 'rep')
- old_down: bfloat16 [2, 4, 1, 8960, 1536], P('side', 'rep')
- prompts: bfloat16 [2, 4, 8192, 1536], P('side', 'rep')
Outputs:
- output 1: float32 [2, 1, 1536, 8960], P('side', None, 'rep')
- output 2: float32 [2, 1, 8960, 1536], P('side', None, None, 'rep')
- output 3: bfloat16 [2, 4, 8192, 1536], P('side', 'rep')
All inputs are finite; a program needn't handle non-finite values.
Results may differ from the reference program's by a relative error of at most 0.001.
Values are sent between devices in bfloat16 or wider.
A program may use at most 1 GiB of HBM per device.

```python
import jax
import jax.numpy as jnp
from jax import lax

MODEL_DIM = 1536
HIDDEN_DIM = 8960
LAYERS = 1
TOKENS = 8192
REPLICAS = 4
TP_WIDTH = 1
SHARD_DIM = HIDDEN_DIM // TP_WIDTH


def split_up(full):
    return jnp.transpose(full.reshape(LAYERS, MODEL_DIM, TP_WIDTH, SHARD_DIM), (2, 0, 1, 3))


def split_down(full):
    return jnp.transpose(full.reshape(LAYERS, TP_WIDTH, SHARD_DIM, MODEL_DIM), (1, 0, 2, 3))


def merge_up(blocks):
    return jnp.transpose(blocks, (1, 2, 0, 3)).reshape(LAYERS, MODEL_DIM, HIDDEN_DIM)


def merge_down(blocks):
    return jnp.transpose(blocks, (1, 0, 2, 3)).reshape(LAYERS, HIDDEN_DIM, MODEL_DIM)


def trainer_slots(blocks):
    return jnp.concatenate([blocks, jnp.zeros_like(blocks)], axis=0)


def generator_slots(blocks):
    copies = jnp.broadcast_to(blocks[:, None], (TP_WIDTH, REPLICAS) + blocks.shape[1:])
    return jnp.concatenate([jnp.zeros_like(copies), copies], axis=0)


def setup_inputs(seed: int = 0) -> dict:
    rng_keys = jax.random.split(jax.random.key(seed), 8)
    up_scale = MODEL_DIM ** -0.5
    down_scale = HIDDEN_DIM ** -0.5
    up_shape = (LAYERS, MODEL_DIM, HIDDEN_DIM)
    down_shape = (LAYERS, HIDDEN_DIM, MODEL_DIM)
    w_up_full = jax.random.normal(rng_keys[0], up_shape, jnp.float32) * up_scale
    w_down_full = jax.random.normal(rng_keys[1], down_shape, jnp.float32) * down_scale
    g_up_full = jax.random.normal(rng_keys[2], up_shape, jnp.float32) * up_scale
    g_down_full = jax.random.normal(rng_keys[3], down_shape, jnp.float32) * down_scale
    learn_rate = jax.random.uniform(rng_keys[4], (1,), jnp.float32, minval=0.15, maxval=0.3)
    stale_up = (w_up_full + 0.2 * up_scale * jax.random.normal(rng_keys[5], up_shape, jnp.float32)).astype(jnp.bfloat16)
    stale_down = (w_down_full + 0.2 * down_scale * jax.random.normal(rng_keys[6], down_shape, jnp.float32)).astype(jnp.bfloat16)
    prompt_rows = jax.random.normal(rng_keys[7], (REPLICAS, TOKENS, MODEL_DIM), jnp.float32).astype(jnp.bfloat16)
    prompt_copies = jnp.broadcast_to(prompt_rows[None], (TP_WIDTH,) + prompt_rows.shape)
    return {
        "w_up": trainer_slots(split_up(w_up_full)),
        "w_down": trainer_slots(split_down(w_down_full)),
        "g_up": trainer_slots(split_up(g_up_full)),
        "g_down": trainer_slots(split_down(g_down_full)),
        "learn_rate": learn_rate,
        "old_up": generator_slots(split_up(stale_up)),
        "old_down": generator_slots(split_down(stale_down)),
        "prompts": jnp.concatenate([jnp.zeros_like(prompt_copies), prompt_copies], axis=0),
    }


def layer_step(hidden, weights):
    up_mat, down_mat = weights
    pre_act = jnp.dot(hidden, up_mat, preferred_element_type=jnp.float32)
    act_val = jax.nn.gelu(pre_act, approximate=False).astype(jnp.bfloat16)
    branch = jnp.dot(act_val, down_mat, preferred_element_type=jnp.float32)
    return (hidden.astype(jnp.float32) + branch).astype(jnp.bfloat16), None


def reference(w_up, w_down, g_up, g_down, learn_rate, old_up, old_down, prompts):
    step_rate = learn_rate[0]
    new_up = w_up - step_rate * g_up
    new_down = w_down - step_rate * g_down
    delta_up = merge_up((new_up - w_up)[:TP_WIDTH].astype(jnp.bfloat16)).astype(jnp.float32)
    delta_down = merge_down((new_down - w_down)[:TP_WIDTH].astype(jnp.bfloat16)).astype(jnp.float32)
    stale_gen_up = jnp.swapaxes(old_up[TP_WIDTH:], 0, 1)
    stale_gen_down = jnp.swapaxes(old_down[TP_WIDTH:], 0, 1)

    def one_replica(operands):
        rep_up, rep_down, rep_x = operands
        gen_up = (merge_up(rep_up).astype(jnp.float32) + delta_up).astype(jnp.bfloat16)
        gen_down = (merge_down(rep_down).astype(jnp.float32) + delta_down).astype(jnp.bfloat16)
        final_h, _ = lax.scan(layer_step, rep_x, (gen_up, gen_down))
        return final_h

    gen_out = lax.map(one_replica, (stale_gen_up, stale_gen_down, prompts[TP_WIDTH]))
    gen_copies = jnp.broadcast_to(gen_out[None], (TP_WIDTH,) + gen_out.shape)
    outputs = jnp.concatenate([jnp.zeros_like(gen_copies), gen_copies], axis=0)
    return new_up, new_down, outputs
```

```python
import jax
import jax.numpy as jnp
from jax import lax
from jax.experimental import pallas as pl
from jax.experimental.pallas import tpu as pltpu
from jax.sharding import PartitionSpec as P

MESH = pl.DeviceIdType.MESH
BF = jnp.bfloat16
F32 = jnp.float32

SMALL, LARGE = 256, 512
N_SMALL = 5
TILE = 1024
TILE_T = 256
VMEM_BYTES = 67043328


def gelu_bf16(v):
    return (0.5 * v * (1.0 + lax.erf(v * 0.7071067811865476))).astype(BF)


def dot(a, b):
    return jnp.dot(a, b, preferred_element_type=F32)


def make_step(D, F, B, reps):
    S = D // reps
    n_large = (F - N_SMALL * SMALL) // LARGE
    assert N_SMALL * SMALL + n_large * LARGE == F
    NCH = N_SMALL + n_large
    base_small = n_large * LARGE
    n_tok_t = TILE
    n_tok_g = B - n_tok_t
    NT = n_tok_g // TILE
    NTT = n_tok_t // TILE_T
    LAST = NCH - 1

    def piece_off(k, fc):
        if fc == SMALL:
            return pl.multiple_of(base_small + k * SMALL, SMALL)
        return pl.multiple_of((k - N_SMALL) * LARGE, LARGE)

    def sized(k, fn):
        if isinstance(k, int):
            if 0 <= k < NCH:
                fn(k, SMALL if k < N_SMALL else LARGE)
            return

        @pl.when(jnp.logical_and(k >= 0, k < N_SMALL))
        def _():
            fn(k, SMALL)

        @pl.when(jnp.logical_and(k >= N_SMALL, k < NCH))
        def _():
            fn(k, LARGE)

    def kern(lr, w_up, w_dn, g_up, g_dn, old_up, old_dn, x,
             q_up, q_dn, pay_up, pay_dn, wg_up, wg_dn, xr, ys, yr, pout,
             p, xb, wub, wdb, sq_up, sq_dn, so_up, so_dn,
             y_s, y_r, x_s, x_r, s_s, s_r, f_s, f_r, xt_s, xt_r, yt_s, yt_r,
             la, lb, lw, lx, lp, l0):
        side = lax.axis_index("side")
        r = lax.axis_index("rep")
        is_gen = side == 1
        peer = (1 - side, r)
        rx = lax.rem(r + 2, 4)
        rs = r + 1 - 2 * lax.rem(r, 2)
        xn = (side, rx)
        sib = (side, rs)

        barrier = pltpu.get_barrier_semaphore()
        for dev in (peer, xn, sib):
            pl.semaphore_signal(barrier, inc=1, device_id=dev, device_id_type=MESH)
        pl.semaphore_wait(barrier, 3)

        def rows(i):
            return pl.ds(pl.multiple_of(i * S, 128), S)

        def local(src, dst, sem):
            return pltpu.make_async_copy(src, dst, sem)

        def remote(src, dst, ss, rs_, dev):
            return pltpu.make_async_remote_copy(
                src_ref=src, dst_ref=dst, send_sem=ss, recv_sem=rs_,
                device_id=dev, device_id_type=MESH)

        def y_copies(k, fc, srcs):
            f = pl.ds(piece_off(k, fc), fc)
            a, b = srcs(f)
            return (remote(a, q_up.at[:, f], y_s.at[k, 0], y_r.at[k, 0], peer),
                    remote(b, q_dn.at[f, :], y_s.at[k, 1], y_r.at[k, 1], peer))

        def gen_src(f):
            return old_up.at[rows(r), f], old_dn.at[f, rows(r)]

        def trn_src(f):
            return pay_up.at[:, f], pay_dn.at[f, :]

        def x_copies(k, fc):
            f = pl.ds(piece_off(k, fc), fc)
            a, b = wg_up.at[rows(r), f], wg_dn.at[f, rows(r)]
            return (remote(a, a, x_s.at[k, 0], x_r.at[k, 0], xn),
                    remote(b, b, x_s.at[k, 1], x_r.at[k, 1], xn))

        def s_copies(k, fc):
            f = pl.ds(piece_off(k, fc), fc)
            a, b = wg_up.at[rows(r), f], wg_dn.at[f, rows(r)]
            return (remote(a, a, s_s.at[k, 0], s_r.at[k, 0], sib),
                    remote(b, b, s_s.at[k, 1], s_r.at[k, 1], sib))

        def f_copies(k, fc):
            f = pl.ds(piece_off(k, fc), fc)
            a, b = wg_up.at[rows(rx), f], wg_dn.at[f, rows(rx)]
            return (remote(a, a, f_s.at[k, 0], f_r.at[k, 0], sib),
                    remote(b, b, f_s.at[k, 1], f_r.at[k, 1], sib))

        def a_copies(k, fc, srcs):
            f = pl.ds(piece_off(k, fc), fc)
            a, b = srcs(f)
            return (local(q_up.at[:, f], sq_up.at[:, pl.ds(0, fc)], la.at[0]),
                    local(q_dn.at[f, :], sq_dn.at[pl.ds(0, fc), :], la.at[1]),
                    local(a, so_up.at[:, pl.ds(0, fc)], la.at[2]),
                    local(b, so_dn.at[pl.ds(0, fc), :], la.at[3]))

        def b_copies(k, fc):
            f = pl.ds(piece_off(k, fc), fc)
            return (local(so_up.at[:, pl.ds(0, fc)], wg_up.at[rows(r), f], lb.at[0]),
                    local(so_dn.at[pl.ds(0, fc), :], wg_dn.at[f, rows(r)], lb.at[1]))

        def step_a(srcs):
            def fn(k, fc):
                for c in y_copies(k, fc, srcs):
                    c.wait_recv()
                for c in a_copies(k, fc, srcs):
                    c.start()
            return fn

        def step_b(srcs):
            def fn(k, fc):
                for c in a_copies(k, fc, srcs):
                    c.wait()
                so_up[:, :fc] = (so_up[:, :fc].astype(F32) + sq_up[:, :fc].astype(F32)).astype(BF)
                so_dn[:fc, :] = (so_dn[:fc, :].astype(F32) + sq_dn[:fc, :].astype(F32)).astype(BF)
                for c in b_copies(k, fc):
                    c.start()
            return fn

        def step_c(k, fc):
            for c in b_copies(k, fc):
                c.wait()
            for c in x_copies(k, fc):
                c.start()
            for c in s_copies(k, fc):
                c.start()

        def step_d(k, fc):
            for c in x_copies(k, fc):
                c.wait_recv()
            for c in f_copies(k, fc):
                c.start()

        def arrive(k, fc):
            for c in s_copies(k, fc):
                c.wait_recv()
            for c in f_copies(k, fc):
                c.wait_recv()

        def w_copies(k, fc, slot):
            f = pl.ds(piece_off(k, fc), fc)
            return (local(wg_up.at[:, f], wub.at[slot, :, pl.ds(0, fc)], lw.at[slot, 0]),
                    local(wg_dn.at[f, :], wdb.at[slot, pl.ds(0, fc), :], lw.at[slot, 1]))

        def w_start(k, fc, slot):
            for c in w_copies(k, fc, slot):
                c.start()

        def w_wait(k, fc, slot):
            for c in w_copies(k, fc, slot):
                c.wait()

        def xt_copy(i):
            return remote(x.at[pl.ds(n_tok_g + i * TILE_T, TILE_T)], xr.at[pl.ds(i * TILE_T, TILE_T)],
                          xt_s.at[i], xt_r.at[i], peer)

        def yt_copy(i):
            return remote(ys.at[pl.ds(i * TILE_T, TILE_T)], yr.at[pl.ds(i * TILE_T, TILE_T)],
                          yt_s.at[i], yt_r.at[i], peer)

        def drain(srcs):
            def fn(k, fc):
                for cs in (y_copies(k, fc, srcs), x_copies(k, fc), s_copies(k, fc), f_copies(k, fc)):
                    for c in cs:
                        c.wait_send()

            @pl.loop(0, NCH)
            def _(k):
                sized(k, fn)

        @pl.when(is_gen)
        def _():
            for k in range(NCH):
                for c in y_copies(k, SMALL if k < N_SMALL else LARGE, gen_src):
                    c.start()
            for i in range(NTT):
                xt_copy(i).start()

            def x_load(t, slot):
                return local(x.at[pl.ds(pl.multiple_of(t * TILE, TILE), TILE)], xb.at[slot], lx.at[slot])

            def p_out(t):
                d = pl.ds(pl.multiple_of(t * TILE, TILE), TILE)
                return local(p.at[d], pout.at[d], lp.at[t])

            x_load(0, 0).start()

            @pl.loop(0, n_tok_g // 256)
            def _(i):
                p[pl.ds(pl.multiple_of(i * 256, 256), 256)] = jnp.zeros((256, D), F32)

            A, Bs = step_a(gen_src), step_b(gen_src)
            for k in range(2):
                sized(k, A)
                sized(k, Bs)
                sized(k, step_c)
            sized(0, step_d)
            arrive(0, SMALL)
            w_start(0, SMALL, 0)

            def tile_math(t, xs, s, fc):
                h = TILE // 2
                base = pl.multiple_of(t * TILE, TILE)
                pre_a = dot(xb[xs, :h], wub[s, :, :fc])
                u_a = gelu_bf16(pre_a)
                pre_b = dot(xb[xs, h:], wub[s, :, :fc])
                p[pl.ds(base, h)] += dot(u_a, wdb[s, :fc, :])
                u_b = gelu_bf16(pre_b)
                p[pl.ds(base + h, h)] += dot(u_b, wdb[s, :fc, :])

            def chunk(c, fc):
                s = lax.rem(c, 2)
                w_wait(c, fc, s)

                @pl.loop(0, NT)
                def _(t):
                    i = c * NT + t
                    xs = lax.rem(i, 2)
                    x_load(t, xs).wait()
                    x_load(lax.rem(t + 1, NT), 1 - xs).start()

                    @pl.when(t == 2)
                    def _():
                        sized(c + 2, A)

                    @pl.when(t == 3)
                    def _():
                        sized(c + 2, Bs)
                        sized(c + 1, step_d)

                    @pl.when(t == 4)
                    def _():
                        sized(c + 2, step_c)

                    @pl.when(t == 5)
                    def _():
                        def load_next(k, fck):
                            arrive(k, fck)

                            @pl.when(k < LAST)
                            def _():
                                w_start(k, fck, 1 - s)
                        sized(c + 1, load_next)

                    tile_math(t, xs, s, fc)

                    @pl.when(c == LAST - 1)
                    def _():
                        p_out(t).start()

            @pl.loop(0, N_SMALL)
            def _(c):
                chunk(c, SMALL)

            @pl.loop(N_SMALL, LAST)
            def _(c):
                chunk(c, LARGE)

            x_load(0, (LAST * NT) % 2).wait()
            for t in range(NT):
                p_out(t).wait()
            for i in range(NTT):
                yt_copy(i).wait_recv()
            drain(gen_src)
            for i in range(NTT):
                xt_copy(i).wait_send()

        @pl.when(jnp.logical_not(is_gen))
        def _():
            rate = lr[0]

            def u_load(k, fc):
                f = pl.ds(piece_off(k, fc), fc)
                return (local(w_up.at[:, f], p.at[pl.ds(0, S), pl.ds(0, fc)], l0.at[0]),
                        local(g_up.at[:, f], p.at[pl.ds(S, S), pl.ds(0, fc)], l0.at[1]),
                        local(w_dn.at[f, :], p.at[pl.ds(2 * S, fc), pl.ds(0, S)], l0.at[2]),
                        local(g_dn.at[f, :], p.at[pl.ds(2 * S + LARGE, fc), pl.ds(0, S)], l0.at[3]))

            def u_store(k, fc):
                f = pl.ds(piece_off(k, fc), fc)
                return (local(wub.at[0, pl.ds(0, S), pl.ds(0, fc)], pay_up.at[:, f], l0.at[4]),
                        local(wdb.at[0, pl.ds(0, fc), pl.ds(0, S)], pay_dn.at[f, :], l0.at[5]))

            def u_start(k, fc):
                for c in u_load(k, fc):
                    c.start()

            def u_math(k, fc):
                for c in u_load(k, fc):
                    c.wait()
                w = p[:S, :fc]
                new = w - rate * p[S:2 * S, :fc]
                wub[0, :S, :fc] = (new - w).astype(BF)
                w = p[2 * S:2 * S + fc, :S]
                new = w - rate * p[2 * S + LARGE:2 * S + LARGE + fc, :S]
                wdb[0, :fc, :S] = (new - w).astype(BF)
                for c in u_store(k, fc):
                    c.start()

            def u_send(k, fc):
                for c in u_store(k, fc):
                    c.wait()
                for c in y_copies(k, fc, trn_src):
                    c.start()

            for k in range(2):
                sized(k, u_start)
                sized(k, u_math)
                sized(k, u_send)
            A, Bs = step_a(trn_src), step_b(trn_src)

            @pl.loop(0, NCH)
            def _(k):
                sized(k + 2, u_start)
                sized(k, A)
                sized(k + 2, u_math)
                sized(k, Bs)
                sized(k + 2, u_send)
                sized(k, step_c)
                sized(k - 1, step_d)

            sized(NCH - 1, step_d)

            def x_load(i):
                return local(xr.at[pl.ds(i * TILE_T, TILE_T)], xb.at[0, pl.ds(0, TILE_T)], lx.at[0])

            def y_out(i):
                return local(xb.at[1, pl.ds(0, TILE_T)], ys.at[pl.ds(i * TILE_T, TILE_T)], lx.at[1])

            arrive(0, SMALL)
            w_start(0, SMALL, 0)

            @pl.loop(0, NTT)
            def _(i):
                xt_copy(i).wait_recv()
                x_load(i).start()
                p[:TILE_T] = jnp.zeros((TILE_T, D), F32)
                x_load(i).wait()

                def piece(k, fc):
                    s = lax.rem(k, 2)
                    w_wait(k, fc, s)

                    def nxt(kn, fcn):
                        @pl.when(i == 0)
                        def _():
                            arrive(kn, fcn)
                        w_start(kn, fcn, 1 - s)
                    sized(k + 1, nxt)

                    @pl.when(jnp.logical_and(k == LAST, i < NTT - 1))
                    def _():
                        w_start(0, SMALL, 1 - s)

                    if fc == SMALL:
                        u = gelu_bf16(dot(xb[0, :TILE_T], wub[s, :, :fc]))
                        p[:TILE_T] += dot(u, wdb[s, :fc, :])
                    else:
                        h = fc // 2
                        pre_a = dot(xb[0, :TILE_T], wub[s, :, :h])
                        u_a = gelu_bf16(pre_a)
                        pre_b = dot(xb[0, :TILE_T], wub[s, :, h:])
                        acc = dot(u_a, wdb[s, :h, :])
                        u_b = gelu_bf16(pre_b)
                        p[:TILE_T] += acc + dot(u_b, wdb[s, h:, :])

                @pl.loop(0, N_SMALL)
                def _(k):
                    piece(k, SMALL)

                @pl.loop(N_SMALL, NCH)
                def _(k):
                    piece(k, LARGE)

                xb[1, :TILE_T] = (xb[0, :TILE_T].astype(F32) + p[:TILE_T]).astype(BF)
                y_out(i).start()
                y_out(i).wait()
                yt_copy(i).start()

            drain(trn_src)
            for i in range(NTT):
                yt_copy(i).wait_send()

    def first(lr, w_up, w_dn, g_up, g_dn, old_up, old_dn, x):
        sds = jax.ShapeDtypeStruct
        outs = (sds((S, F), BF), sds((F, S), BF), sds((S, F), BF), sds((F, S), BF),
                sds((D, F), BF), sds((F, D), BF),
                sds((n_tok_t, D), BF), sds((n_tok_t, D), BF), sds((n_tok_t, D), BF),
                sds((n_tok_g, D), F32))
        dma = pltpu.SemaphoreType.DMA
        anyspace = pl.BlockSpec(memory_space=pl.ANY)
        return pl.pallas_call(
            kern,
            out_shape=outs,
            in_specs=[pl.BlockSpec(memory_space=pltpu.SMEM)] + [anyspace] * 7,
            out_specs=[anyspace] * len(outs),
            scratch_shapes=[
                pltpu.VMEM((n_tok_g, D), F32),
                pltpu.VMEM((2, TILE, D), BF),
                pltpu.VMEM((2, D, LARGE), BF),
                pltpu.VMEM((2, LARGE, D), BF),
                pltpu.VMEM((S, LARGE), BF), pltpu.VMEM((LARGE, S), BF),
                pltpu.VMEM((S, LARGE), BF), pltpu.VMEM((LARGE, S), BF),
            ] + [dma((NCH, 2))] * 8 + [dma((NTT,))] * 4 + [
                dma((4,)), dma((2,)), dma((2, 2)), dma((2,)), dma((NT,)), dma((6,)),
            ],
            compiler_params=pltpu.CompilerParams(
                collective_id=0, has_side_effects=True, vmem_limit_bytes=VMEM_BYTES),
            name="sync_and_mlp",
        )(lr, w_up, w_dn, g_up, g_dn, old_up, old_dn, x)

    def kern2(x_ref, p_ref, wu_ref, wd_ref, yr_ref, y_ref):
        t = pl.program_id(0)
        is_gen = lax.axis_index("side") == 1

        @pl.when(jnp.logical_not(is_gen))
        def _():
            y_ref[...] = jnp.zeros_like(y_ref)

        @pl.when(jnp.logical_and(is_gen, t == NT))
        def _():
            y_ref[...] = yr_ref[...]

        @pl.when(jnp.logical_and(is_gen, t < NT))
        def _():
            h = TILE // 2
            pre_a = dot(x_ref[:h], wu_ref[...])
            u_a = gelu_bf16(pre_a)
            pre_b = dot(x_ref[h:], wu_ref[...])
            y_ref[:h] = (x_ref[:h].astype(F32) + (p_ref[:h] + dot(u_a, wd_ref[...]))).astype(BF)
            u_b = gelu_bf16(pre_b)
            y_ref[h:] = (x_ref[h:].astype(F32) + (p_ref[h:] + dot(u_b, wd_ref[...]))).astype(BF)

    def second(x, pout, wg_up, wg_dn, yr):
        jl = n_large - 1
        return pl.pallas_call(
            kern2,
            out_shape=jax.ShapeDtypeStruct((B, D), BF),
            grid=(NT + 1,),
            in_specs=[
                pl.BlockSpec((TILE, D), lambda t: (t, 0)),
                pl.BlockSpec((TILE, D), lambda t: (jnp.minimum(t, NT - 1), 0)),
                pl.BlockSpec((D, LARGE), lambda t: (0, jl)),
                pl.BlockSpec((LARGE, D), lambda t: (jl, 0)),
                pl.BlockSpec((n_tok_t, D), lambda t: (0, 0)),
            ],
            out_specs=pl.BlockSpec((TILE, D), lambda t: (t, 0)),
            compiler_params=pltpu.CompilerParams(vmem_limit_bytes=VMEM_BYTES),
            name="last_piece",
        )(x, pout, wg_up, wg_dn, yr)

    return first, second


def solution(mesh):
    reps = mesh.shape["rep"]
    up_spec = P("side", None, "rep", None)
    down_spec = P("side", None, None, "rep")
    copy_spec = P("side", "rep", None, None, None)
    token_spec = P("side", "rep", None, None)

    def local_step(w_up, w_down, g_up, g_down, learn_rate, old_up, old_down, prompts):
        B, D = prompts.shape[2:]
        F = w_up.shape[3]
        first, second = make_step(D, F, B, reps)
        x = prompts[0, 0]
        outs = first(learn_rate, w_up[0, 0], w_down[0, 0], g_up[0, 0], g_down[0, 0],
                     old_up[0, 0, 0], old_down[0, 0, 0], x)
        wg_up, wg_dn, yr, pout = outs[4], outs[5], outs[8], outs[9]
        y = second(x, pout, wg_up, wg_dn, yr)
        new_up = w_up - learn_rate[0] * g_up
        new_down = w_down - learn_rate[0] * g_down
        return new_up, new_down, y[None, None]

    return jax.shard_map(
        local_step,
        mesh=mesh,
        in_specs=(up_spec, down_spec, up_spec, down_spec, P(None), copy_spec, copy_spec, token_spec),
        out_specs=(up_spec, down_spec, token_spec),
        check_vma=False,
    )
```

```python
import jax
import jax.numpy as jnp
from jax import lax
from jax.experimental import pallas as pl
from jax.experimental.pallas import tpu as pltpu
from jax.sharding import PartitionSpec as P

MESH = pl.DeviceIdType.MESH
BF = jnp.bfloat16
F32 = jnp.float32

SMALL, LARGE = 256, 512
N_SMALL = 5
TILE = 1024
TILE_T = 256
LEAD_T = 5
DEPTH = 4
N_SECOND = 2
VMEM_BYTES = 67043328


def gelu_bf16(v):
    return (0.5 * v * (1.0 + lax.erf(v * 0.7071067811865476))).astype(BF)


def dot(a, b):
    return jnp.dot(a, b, preferred_element_type=F32)


def make_step(D, F, B, reps):
    S = D // reps
    n_large = (F - N_SMALL * SMALL) // LARGE
    assert N_SMALL * SMALL + n_large * LARGE == F
    NCH = N_SMALL + n_large
    base_small = n_large * LARGE
    n_tok_t = TILE
    n_tok_g = B - n_tok_t
    NT = n_tok_g // TILE
    NTT = n_tok_t // TILE_T
    N_FIRST = NCH - N_SECOND

    def piece_off(k, fc):
        if fc == SMALL:
            return pl.multiple_of(base_small + k * SMALL, SMALL)
        return pl.multiple_of((NCH - 1 - k) * LARGE, LARGE)

    def sized(k, fn):
        if isinstance(k, int):
            if 0 <= k < NCH:
                fn(k, SMALL if k < N_SMALL else LARGE)
            return

        @pl.when(jnp.logical_and(k >= 0, k < N_SMALL))
        def _():
            fn(k, SMALL)

        @pl.when(jnp.logical_and(k >= N_SMALL, k < NCH))
        def _():
            fn(k, LARGE)

    def kern(lr, w_up, w_dn, g_up, g_dn, old_up, old_dn, x,
             q_up, q_dn, pay_up, pay_dn, wg_up, wg_dn, xr, ys, yr, pout,
             sq_up, sq_dn, so_up, so_dn,
             y_s, y_r, x_s, x_r, s_s, s_r, f_s, f_r, xt_s, xt_r, yt_s, yt_r,
             la, lb, lw, lx, lp, l0):
        side = lax.axis_index("side")
        r = lax.axis_index("rep")
        is_gen = side == 1
        peer = (1 - side, r)
        rx = lax.rem(r + 2, 4)
        rs = r + 1 - 2 * lax.rem(r, 2)
        xn = (side, rx)
        sib = (side, rs)

        barrier = pltpu.get_barrier_semaphore()
        for dev in (peer, xn, sib):
            pl.semaphore_signal(barrier, inc=1, device_id=dev, device_id_type=MESH)
        pl.semaphore_wait(barrier, 3)

        def rows(i):
            return pl.ds(pl.multiple_of(i * S, 128), S)

        def local(src, dst, sem):
            return pltpu.make_async_copy(src, dst, sem)

        def remote(src, dst, ss, rs_, dev):
            return pltpu.make_async_remote_copy(
                src_ref=src, dst_ref=dst, send_sem=ss, recv_sem=rs_,
                device_id=dev, device_id_type=MESH)

        def y_copies(k, fc, srcs):
            f = pl.ds(piece_off(k, fc), fc)
            a, b = srcs(f)
            return (remote(a, q_up.at[:, f], y_s.at[k, 0], y_r.at[k, 0], peer),
                    remote(b, q_dn.at[f, :], y_s.at[k, 1], y_r.at[k, 1], peer))

        def gen_src(f):
            return old_up.at[rows(r), f], old_dn.at[f, rows(r)]

        def trn_src(f):
            return pay_up.at[:, f], pay_dn.at[f, :]

        def x_copies(k, fc):
            f = pl.ds(piece_off(k, fc), fc)
            a, b = wg_up.at[rows(r), f], wg_dn.at[f, rows(r)]
            return (remote(a, a, x_s.at[k, 0], x_r.at[k, 0], xn),
                    remote(b, b, x_s.at[k, 1], x_r.at[k, 1], xn))

        def s_copies(k, fc):
            f = pl.ds(piece_off(k, fc), fc)
            a, b = wg_up.at[rows(r), f], wg_dn.at[f, rows(r)]
            return (remote(a, a, s_s.at[k, 0], s_r.at[k, 0], sib),
                    remote(b, b, s_s.at[k, 1], s_r.at[k, 1], sib))

        def f_copies(k, fc):
            f = pl.ds(piece_off(k, fc), fc)
            a, b = wg_up.at[rows(rx), f], wg_dn.at[f, rows(rx)]
            return (remote(a, a, f_s.at[k, 0], f_r.at[k, 0], sib),
                    remote(b, b, f_s.at[k, 1], f_r.at[k, 1], sib))

        def a_copies(k, fc, srcs):
            f = pl.ds(piece_off(k, fc), fc)
            a, b = srcs(f)
            return (local(q_up.at[:, f], sq_up.at[:, pl.ds(0, fc)], la.at[0]),
                    local(q_dn.at[f, :], sq_dn.at[pl.ds(0, fc), :], la.at[1]),
                    local(a, so_up.at[:, pl.ds(0, fc)], la.at[2]),
                    local(b, so_dn.at[pl.ds(0, fc), :], la.at[3]))

        def b_copies(k, fc):
            f = pl.ds(piece_off(k, fc), fc)
            return (local(so_up.at[:, pl.ds(0, fc)], wg_up.at[rows(r), f], lb.at[0]),
                    local(so_dn.at[pl.ds(0, fc), :], wg_dn.at[f, rows(r)], lb.at[1]))

        def step_a(srcs):
            def fn(k, fc):
                for c in y_copies(k, fc, srcs):
                    c.wait_recv()
                for c in a_copies(k, fc, srcs):
                    c.start()
            return fn

        def step_b(srcs):
            def fn(k, fc):
                for c in a_copies(k, fc, srcs):
                    c.wait()
                so_up[:, :fc] = (so_up[:, :fc].astype(F32) + sq_up[:, :fc].astype(F32)).astype(BF)
                so_dn[:fc, :] = (so_dn[:fc, :].astype(F32) + sq_dn[:fc, :].astype(F32)).astype(BF)
                for c in b_copies(k, fc):
                    c.start()
            return fn

        def step_c(k, fc):
            for c in b_copies(k, fc):
                c.wait()
            for c in x_copies(k, fc):
                c.start()
            for c in s_copies(k, fc):
                c.start()

        def step_d(k, fc):
            for c in x_copies(k, fc):
                c.wait_recv()
            for c in f_copies(k, fc):
                c.start()

        def arrive(k, fc):
            for c in s_copies(k, fc):
                c.wait_recv()
            for c in f_copies(k, fc):
                c.wait_recv()

        def w_stream(wub, wdb):
            def copies(k, fc, slot):
                f = pl.ds(piece_off(k, fc), fc)
                return (local(wg_up.at[:, f], wub.at[slot, :, pl.ds(0, fc)], lw.at[slot, 0]),
                        local(wg_dn.at[f, :], wdb.at[slot, pl.ds(0, fc), :], lw.at[slot, 1]))

            def start(k, fc, slot):
                for c in copies(k, fc, slot):
                    c.start()

            def wait(k, fc, slot):
                for c in copies(k, fc, slot):
                    c.wait()
            return start, wait

        def xt_copy(i):
            return remote(x.at[pl.ds(n_tok_g + i * TILE_T, TILE_T)], xr.at[pl.ds(i * TILE_T, TILE_T)],
                          xt_s.at[i], xt_r.at[i], peer)

        def yt_copy(i):
            return remote(ys.at[pl.ds(i * TILE_T, TILE_T)], yr.at[pl.ds(i * TILE_T, TILE_T)],
                          yt_s.at[i], yt_r.at[i], peer)

        def drain(srcs):
            def fn(k, fc):
                for cs in (y_copies(k, fc, srcs), x_copies(k, fc), s_copies(k, fc), f_copies(k, fc)):
                    for c in cs:
                        c.wait_send()

            @pl.loop(0, NCH)
            def _(k):
                sized(k, fn)

        def generator(p, xb, wub, wdb):
            w_start, w_wait = w_stream(wub, wdb)
            for k in range(NCH):
                for c in y_copies(k, SMALL if k < N_SMALL else LARGE, gen_src):
                    c.start()
            for i in range(NTT):
                xt_copy(i).start()

            def x_load(t, slot):
                return local(x.at[pl.ds(pl.multiple_of(t * TILE, TILE), TILE)], xb.at[slot], lx.at[slot])

            def p_out(t):
                d = pl.ds(pl.multiple_of(t * TILE, TILE), TILE)
                return local(p.at[d], pout.at[d], lp.at[t])

            x_load(0, 0).start()

            @pl.loop(0, n_tok_g // 256)
            def _(i):
                p[pl.ds(pl.multiple_of(i * 256, 256), 256)] = jnp.zeros((256, D), F32)

            A, Bs = step_a(gen_src), step_b(gen_src)
            for k in range(2):
                sized(k, A)
                sized(k, Bs)
                sized(k, step_c)
            sized(0, step_d)
            arrive(0, SMALL)
            w_start(0, SMALL, 0)

            def tile_math(t, xs, s, fc):
                h = TILE // 2
                base = pl.multiple_of(t * TILE, TILE)
                pre_a = dot(xb[xs, :h], wub[s, :, :fc])
                u_a = gelu_bf16(pre_a)
                pre_b = dot(xb[xs, h:], wub[s, :, :fc])
                p[pl.ds(base, h)] += dot(u_a, wdb[s, :fc, :])
                u_b = gelu_bf16(pre_b)
                p[pl.ds(base + h, h)] += dot(u_b, wdb[s, :fc, :])

            def chunk(c, fc, sized):
                s = lax.rem(c, 2)
                w_wait(c, fc, s)

                @pl.loop(0, NT)
                def _(t):
                    i = c * NT + t
                    xs = lax.rem(i, 2)
                    x_load(t, xs).wait()
                    x_load(lax.rem(t + 1, NT), 1 - xs).start()

                    @pl.when(t == 0)
                    def _():
                        sized(c + 2, A)

                    @pl.when(t == 1)
                    def _():
                        sized(c + 2, Bs)

                    @pl.when(t == 2)
                    def _():
                        sized(c + 2, step_c)

                    @pl.when(t == 4)
                    def _():
                        sized(c + 1, step_d)

                    @pl.when(t == 6)
                    def _():
                        def load_next(k, fck):
                            arrive(k, fck)

                            @pl.when(k < N_FIRST)
                            def _():
                                w_start(k, fck, 1 - s)
                        sized(c + 1, load_next)

                    tile_math(t, xs, s, fc)

                    @pl.when(c == N_FIRST - 1)
                    def _():
                        p_out(t).start()

            @pl.loop(0, N_SMALL)
            def _(c):
                chunk(c, SMALL, sized)

            @pl.loop(N_SMALL, N_FIRST)
            def _(c):
                chunk(c, LARGE, lambda k, fn: fn(k, LARGE))

            x_load(0, (N_FIRST * NT) % 2).wait()
            for k in range(N_FIRST + 1, NCH):
                sized(k, step_d)
                sized(k, arrive)
            for t in range(NT):
                p_out(t).wait()
            for i in range(NTT):
                yt_copy(i).wait_recv()
            drain(gen_src)
            for i in range(NTT):
                xt_copy(i).wait_send()

        def trainer(p, st, xb, wub, wdb):
            w_start, w_wait = w_stream(wub, wdb)
            rate = lr[0]

            def u_load(k, fc):
                f = pl.ds(piece_off(k, fc), fc)
                return (local(w_up.at[:, f], st.at[pl.ds(0, S), pl.ds(0, fc)], l0.at[0]),
                        local(g_up.at[:, f], st.at[pl.ds(S, S), pl.ds(0, fc)], l0.at[1]),
                        local(w_dn.at[f, :], st.at[pl.ds(2 * S, fc), pl.ds(0, S)], l0.at[2]),
                        local(g_dn.at[f, :], st.at[pl.ds(2 * S + LARGE, fc), pl.ds(0, S)], l0.at[3]))

            def u_store(k, fc):
                f = pl.ds(piece_off(k, fc), fc)
                return (local(wub.at[0, pl.ds(0, S), pl.ds(0, fc)], pay_up.at[:, f], l0.at[4]),
                        local(wdb.at[0, pl.ds(0, fc), pl.ds(0, S)], pay_dn.at[f, :], l0.at[5]))

            def u_start(k, fc):
                for c in u_load(k, fc):
                    c.start()

            def u_math(k, fc):
                for c in u_load(k, fc):
                    c.wait()
                w = st[:S, :fc]
                new = w - rate * st[S:2 * S, :fc]
                wub[0, :S, :fc] = (new - w).astype(BF)
                w = st[2 * S:2 * S + fc, :S]
                new = w - rate * st[2 * S + LARGE:2 * S + LARGE + fc, :S]
                wdb[0, :fc, :S] = (new - w).astype(BF)
                for c in u_store(k, fc):
                    c.start()

            def u_send(k, fc):
                for c in u_store(k, fc):
                    c.wait()
                for c in y_copies(k, fc, trn_src):
                    c.start()

            for k in range(LEAD_T):
                sized(k, u_start)
                sized(k, u_math)
                sized(k, u_send)
            A, Bs = step_a(trn_src), step_b(trn_src)

            @pl.loop(0, NCH)
            def _(k):
                sized(k + LEAD_T, u_start)
                sized(k, A)
                sized(k + LEAD_T, u_math)
                sized(k, Bs)
                sized(k + LEAD_T, u_send)
                sized(k, step_c)
                sized(k - 1, step_d)

            sized(NCH - 1, step_d)

            def x_load(i):
                return local(xr.at[pl.ds(i * TILE_T, TILE_T)], xb.at[0], lx.at[0])

            def y_out(i):
                return local(xb.at[1], ys.at[pl.ds(i * TILE_T, TILE_T)], lx.at[1])

            for k in range(DEPTH - 1):
                arrive(k, SMALL)
                w_start(k, SMALL, k)

            @pl.loop(0, NTT)
            def _(i):
                xt_copy(i).wait_recv()
                x_load(i).start()
                p[...] = jnp.zeros((TILE_T, D), F32)
                x_load(i).wait()

                def piece(k, fc):
                    s = lax.rem(k, DEPTH)
                    w_wait(k, fc, s)
                    ahead = lax.rem(k + DEPTH - 1, DEPTH)

                    def nxt(kn, fcn):
                        @pl.when(i == 0)
                        def _():
                            arrive(kn, fcn)
                        w_start(kn, fcn, ahead)
                    sized(k + DEPTH - 1, nxt)

                    @pl.when(jnp.logical_and(k + DEPTH - 1 >= NCH, i < NTT - 1))
                    def _():
                        w_start(k + DEPTH - 1 - NCH, SMALL, ahead)

                    trainer_math(p, xb, wub, wdb, s, fc)

                @pl.loop(0, N_SMALL)
                def _(k):
                    piece(k, SMALL)

                @pl.loop(N_SMALL, NCH)
                def _(k):
                    piece(k, LARGE)

                xb[1] = (xb[0].astype(F32) + p[...]).astype(BF)
                y_out(i).start()
                y_out(i).wait()
                yt_copy(i).start()

            drain(trn_src)
            for i in range(NTT):
                yt_copy(i).wait_send()

        @pl.when(is_gen)
        def _():
            pl.run_scoped(generator, pltpu.VMEM((n_tok_g, D), F32), pltpu.VMEM((2, TILE, D), BF),
                          pltpu.VMEM((2, D, LARGE), BF), pltpu.VMEM((2, LARGE, D), BF))

        @pl.when(jnp.logical_not(is_gen))
        def _():
            pl.run_scoped(trainer, pltpu.VMEM((TILE_T, D), F32), pltpu.VMEM((2 * S + 2 * LARGE, LARGE), F32),
                          pltpu.VMEM((2, TILE_T, D), BF),
                          pltpu.VMEM((DEPTH, D, LARGE), BF), pltpu.VMEM((DEPTH, LARGE, D), BF))

    def trainer_math(p, xb, wub, wdb, s, fc):
        h = TILE_T // 2
        pre_a = dot(xb[0, :h], wub[s, :, :fc])
        u_a = gelu_bf16(pre_a)
        pre_b = dot(xb[0, h:], wub[s, :, :fc])
        p[:h] += dot(u_a, wdb[s, :fc, :])
        u_b = gelu_bf16(pre_b)
        p[h:] += dot(u_b, wdb[s, :fc, :])

    def first(lr, w_up, w_dn, g_up, g_dn, old_up, old_dn, x):
        sds = jax.ShapeDtypeStruct
        outs = (sds((S, F), BF), sds((F, S), BF), sds((S, F), BF), sds((F, S), BF),
                sds((D, F), BF), sds((F, D), BF),
                sds((n_tok_t, D), BF), sds((n_tok_t, D), BF), sds((n_tok_t, D), BF),
                sds((n_tok_g, D), F32))
        dma = pltpu.SemaphoreType.DMA
        anyspace = pl.BlockSpec(memory_space=pl.ANY)
        return pl.pallas_call(
            kern,
            out_shape=outs,
            in_specs=[pl.BlockSpec(memory_space=pltpu.SMEM)] + [anyspace] * 7,
            out_specs=[anyspace] * len(outs),
            scratch_shapes=[
                pltpu.VMEM((S, LARGE), BF), pltpu.VMEM((LARGE, S), BF),
                pltpu.VMEM((S, LARGE), BF), pltpu.VMEM((LARGE, S), BF),
            ] + [dma((NCH, 2))] * 8 + [dma((NTT,))] * 4 + [
                dma((4,)), dma((2,)), dma((DEPTH, 2)), dma((2,)), dma((NT,)), dma((6,)),
            ],
            compiler_params=pltpu.CompilerParams(
                collective_id=0, has_side_effects=True, vmem_limit_bytes=VMEM_BYTES),
            name="sync_and_mlp",
        )(lr, w_up, w_dn, g_up, g_dn, old_up, old_dn, x)

    bu, bd = S // (NT + 1), F // (NT + 1)

    def kern2(role, lr, x_ref, p_ref, wu_ref, wd_ref, yr_ref, w_up, g_up, w_dn, g_dn,
              y_ref, new_up, new_dn, uw, ug, dw, dg, sem):
        t = pl.program_id(0)
        is_gen = lax.axis_index("side") == 1

        def in_copies():
            u, d = pl.ds(t * bu, bu), pl.ds(t * bd, bd)
            return (pltpu.make_async_copy(w_up.at[u], uw, sem.at[0]),
                    pltpu.make_async_copy(g_up.at[u], ug, sem.at[1]),
                    pltpu.make_async_copy(w_dn.at[d], dw, sem.at[2]),
                    pltpu.make_async_copy(g_dn.at[d], dg, sem.at[3]))

        def out_copies():
            u, d = pl.ds(t * bu, bu), pl.ds(t * bd, bd)
            return (pltpu.make_async_copy(uw, new_up.at[u], sem.at[4]),
                    pltpu.make_async_copy(dw, new_dn.at[d], sem.at[5]))

        @pl.when(jnp.logical_not(is_gen))
        def _():
            for c in in_copies():
                c.start()
            y_ref[...] = jnp.zeros_like(y_ref)
            for c in in_copies():
                c.wait()
            uw[...] = uw[...] - lr[0] * ug[...]
            dw[...] = dw[...] - lr[0] * dg[...]
            for c in out_copies():
                c.start()
            for c in out_copies():
                c.wait()

        @pl.when(is_gen)
        def _():
            @pl.when(t == 0)
            def _():
                uw[...] = jnp.zeros_like(uw)
                dw[...] = jnp.zeros_like(dw)

            for c in out_copies():
                c.start()

        @pl.when(is_gen & (t == NT))
        def _():
            y_ref[...] = yr_ref[...]

        @pl.when(is_gen & (t < NT))
        def _():
            h = TILE // 2
            pre_a = dot(x_ref[:h], wu_ref[...])
            u_a = gelu_bf16(pre_a)
            pre_b = dot(x_ref[h:], wu_ref[...])
            y_ref[:h] = (x_ref[:h].astype(F32) + (p_ref[:h] + dot(u_a, wd_ref[...]))).astype(BF)
            u_b = gelu_bf16(pre_b)
            y_ref[h:] = (x_ref[h:].astype(F32) + (p_ref[h:] + dot(u_b, wd_ref[...]))).astype(BF)

        @pl.when(is_gen)
        def _():
            for c in out_copies():
                c.wait()

    def second(role, lr, x, pout, wg_up, wg_dn, yr, w_up, g_up, w_dn, g_dn):
        fs = N_SECOND * LARGE
        assert bu * (NT + 1) == S and bd * (NT + 1) == F and bu % 8 == 0 and bd % 8 == 0
        once = pl.Buffered(1)
        anyspace = pl.BlockSpec(memory_space=pl.ANY)
        return pl.pallas_call(
            kern2,
            out_shape=(jax.ShapeDtypeStruct((B, D), BF),
                       jax.ShapeDtypeStruct((S, F), F32), jax.ShapeDtypeStruct((F, S), F32)),
            grid_spec=pltpu.PrefetchScalarGridSpec(
                num_scalar_prefetch=1,
                grid=(NT + 1,),
                in_specs=[
                    pl.BlockSpec(memory_space=pltpu.SMEM),
                    pl.BlockSpec((TILE, D), lambda t, role: (jnp.minimum(t, NT - 1) * role[0], 0)),
                    pl.BlockSpec((TILE, D), lambda t, role: (jnp.minimum(t, NT - 1) * role[0], 0)),
                    pl.BlockSpec((D, fs), lambda t, role: (0, 0), pipeline_mode=once),
                    pl.BlockSpec((fs, D), lambda t, role: (0, 0), pipeline_mode=once),
                    pl.BlockSpec((n_tok_t, D), lambda t, role: (0, 0), pipeline_mode=once),
                ] + [anyspace] * 4,
                out_specs=[pl.BlockSpec((TILE, D), lambda t, role: (t, 0)), anyspace, anyspace],
                scratch_shapes=[
                    pltpu.VMEM((bu, F), F32), pltpu.VMEM((bu, F), F32),
                    pltpu.VMEM((bd, S), F32), pltpu.VMEM((bd, S), F32),
                    pltpu.SemaphoreType.DMA((6,)),
                ],
            ),
            compiler_params=pltpu.CompilerParams(vmem_limit_bytes=VMEM_BYTES),
            name="last_pieces",
        )(role, lr, x, pout, wg_up, wg_dn, yr, w_up, g_up, w_dn, g_dn)

    return first, second


def solution(mesh):
    reps = mesh.shape["rep"]
    up_spec = P("side", None, "rep", None)
    down_spec = P("side", None, None, "rep")
    copy_spec = P("side", "rep", None, None, None)
    token_spec = P("side", "rep", None, None)

    def local_step(w_up, w_down, g_up, g_down, learn_rate, old_up, old_down, prompts):
        B, D = prompts.shape[2:]
        F = w_up.shape[3]
        first, second = make_step(D, F, B, reps)
        x = prompts[0, 0]
        outs = first(learn_rate, w_up[0, 0], w_down[0, 0], g_up[0, 0], g_down[0, 0],
                     old_up[0, 0, 0], old_down[0, 0, 0], x)
        wg_up, wg_dn, yr, pout = outs[4], outs[5], outs[8], outs[9]
        role = lax.axis_index("side").astype(jnp.int32)[None]
        y, new_up, new_down = second(role, learn_rate, x, pout, wg_up, wg_dn, yr,
                                     w_up[0, 0], g_up[0, 0], w_down[0, 0], g_down[0, 0])
        return new_up[None, None], new_down[None, None], y[None, None]

    return jax.shard_map(
        local_step,
        mesh=mesh,
        in_specs=(up_spec, down_spec, up_spec, down_spec, P(None), copy_spec, copy_spec, token_spec),
        out_specs=(up_spec, down_spec, token_spec),
        check_vma=False,
    )
```

```python
import jax
import jax.numpy as jnp
from jax import lax
from jax.experimental import pallas as pl
from jax.experimental.pallas import tpu as pltpu
from jax.sharding import PartitionSpec as P

MESH = pl.DeviceIdType.MESH
BF = jnp.bfloat16
F32 = jnp.float32

SMALL, LARGE = 256, 512
N_SMALL = 5
TILE = 1024
TILE_T = 256
LEAD_T = 5
DEPTH = 4
N_SECOND = 2
VMEM_BYTES = 67043328


def gelu_bf16(v):
    return (0.5 * v * (1.0 + lax.erf(v * 0.7071067811865476))).astype(BF)


def dot(a, b):
    return jnp.dot(a, b, preferred_element_type=F32)


def make_step(D, F, B, reps):
    S = D // reps
    n_large = (F - N_SMALL * SMALL) // LARGE
    assert N_SMALL * SMALL + n_large * LARGE == F
    NCH = N_SMALL + n_large
    base_small = n_large * LARGE
    n_tok_t = TILE
    n_tok_g = B - n_tok_t
    NT = n_tok_g // TILE
    NTT = n_tok_t // TILE_T
    N_FIRST = NCH - N_SECOND

    def piece_off(k, fc):
        if fc == SMALL:
            return pl.multiple_of(base_small + k * SMALL, SMALL)
        return pl.multiple_of((NCH - 1 - k) * LARGE, LARGE)

    def sized(k, fn):
        if isinstance(k, int):
            if 0 <= k < NCH:
                fn(k, SMALL if k < N_SMALL else LARGE)
            return

        @pl.when(jnp.logical_and(k >= 0, k < N_SMALL))
        def _():
            fn(k, SMALL)

        @pl.when(jnp.logical_and(k >= N_SMALL, k < NCH))
        def _():
            fn(k, LARGE)

    def kern(lr, w_up, w_dn, g_up, g_dn, old_up, old_dn, x,
             q_up, q_dn, pay_up, pay_dn, wg_up, wg_dn, xr, ys, yr, pout,
             sq_up, sq_dn, so_up, so_dn,
             y_s, y_r, x_s, x_r, s_s, s_r, f_s, f_r, xt_s, xt_r, yt_s, yt_r,
             la, lb, lw, lx, lp, l0):
        side = lax.axis_index("side")
        r = lax.axis_index("rep")
        is_gen = side == 1
        peer = (1 - side, r)
        rx = lax.rem(r + 2, 4)
        rs = r + 1 - 2 * lax.rem(r, 2)
        xn = (side, rx)
        sib = (side, rs)

        barrier = pltpu.get_barrier_semaphore()
        for dev in (peer, xn, sib):
            pl.semaphore_signal(barrier, inc=1, device_id=dev, device_id_type=MESH)
        pl.semaphore_wait(barrier, 3)

        def rows(i):
            return pl.ds(pl.multiple_of(i * S, 128), S)

        def local(src, dst, sem):
            return pltpu.make_async_copy(src, dst, sem)

        def remote(src, dst, ss, rs_, dev):
            return pltpu.make_async_remote_copy(
                src_ref=src, dst_ref=dst, send_sem=ss, recv_sem=rs_,
                device_id=dev, device_id_type=MESH)

        def y_copies(k, fc, srcs):
            f = pl.ds(piece_off(k, fc), fc)
            a, b = srcs(f)
            return (remote(a, q_up.at[:, f], y_s.at[k, 0], y_r.at[k, 0], peer),
                    remote(b, q_dn.at[f, :], y_s.at[k, 1], y_r.at[k, 1], peer))

        def gen_src(f):
            return old_up.at[rows(r), f], old_dn.at[f, rows(r)]

        def trn_src(f):
            return pay_up.at[:, f], pay_dn.at[f, :]

        def x_copies(k, fc):
            f = pl.ds(piece_off(k, fc), fc)
            a, b = wg_up.at[rows(r), f], wg_dn.at[f, rows(r)]
            return (remote(a, a, x_s.at[k, 0], x_r.at[k, 0], xn),
                    remote(b, b, x_s.at[k, 1], x_r.at[k, 1], xn))

        def s_copies(k, fc):
            f = pl.ds(piece_off(k, fc), fc)
            a, b = wg_up.at[rows(r), f], wg_dn.at[f, rows(r)]
            return (remote(a, a, s_s.at[k, 0], s_r.at[k, 0], sib),
                    remote(b, b, s_s.at[k, 1], s_r.at[k, 1], sib))

        def f_copies(k, fc):
            f = pl.ds(piece_off(k, fc), fc)
            a, b = wg_up.at[rows(rx), f], wg_dn.at[f, rows(rx)]
            return (remote(a, a, f_s.at[k, 0], f_r.at[k, 0], sib),
                    remote(b, b, f_s.at[k, 1], f_r.at[k, 1], sib))

        def a_copies(k, fc, srcs):
            f = pl.ds(piece_off(k, fc), fc)
            a, b = srcs(f)
            return (local(q_up.at[:, f], sq_up.at[:, pl.ds(0, fc)], la.at[0]),
                    local(q_dn.at[f, :], sq_dn.at[pl.ds(0, fc), :], la.at[1]),
                    local(a, so_up.at[:, pl.ds(0, fc)], la.at[2]),
                    local(b, so_dn.at[pl.ds(0, fc), :], la.at[3]))

        def b_copies(k, fc):
            f = pl.ds(piece_off(k, fc), fc)
            return (local(so_up.at[:, pl.ds(0, fc)], wg_up.at[rows(r), f], lb.at[0]),
                    local(so_dn.at[pl.ds(0, fc), :], wg_dn.at[f, rows(r)], lb.at[1]))

        def step_a(srcs):
            def fn(k, fc):
                for c in y_copies(k, fc, srcs):
                    c.wait_recv()
                for c in a_copies(k, fc, srcs):
                    c.start()
            return fn

        def step_b(srcs):
            def fn(k, fc):
                for c in a_copies(k, fc, srcs):
                    c.wait()
                so_up[:, :fc] = (so_up[:, :fc].astype(F32) + sq_up[:, :fc].astype(F32)).astype(BF)
                so_dn[:fc, :] = (so_dn[:fc, :].astype(F32) + sq_dn[:fc, :].astype(F32)).astype(BF)
                for c in b_copies(k, fc):
                    c.start()
            return fn

        def step_c(k, fc):
            for c in b_copies(k, fc):
                c.wait()
            for c in x_copies(k, fc):
                c.start()
            for c in s_copies(k, fc):
                c.start()

        def step_d(k, fc):
            for c in x_copies(k, fc):
                c.wait_recv()
            for c in f_copies(k, fc):
                c.start()

        def arrive(k, fc):
            for c in s_copies(k, fc):
                c.wait_recv()
            for c in f_copies(k, fc):
                c.wait_recv()

        def w_stream(wub, wdb):
            def copies(k, fc, slot):
                f = pl.ds(piece_off(k, fc), fc)
                return (local(wg_up.at[:, f], wub.at[slot, :, pl.ds(0, fc)], lw.at[slot, 0]),
                        local(wg_dn.at[f, :], wdb.at[slot, pl.ds(0, fc), :], lw.at[slot, 1]))

            def start(k, fc, slot):
                for c in copies(k, fc, slot):
                    c.start()

            def wait(k, fc, slot):
                for c in copies(k, fc, slot):
                    c.wait()
            return start, wait

        def xt_copy(i):
            return remote(x.at[pl.ds(n_tok_g + i * TILE_T, TILE_T)], xr.at[pl.ds(i * TILE_T, TILE_T)],
                          xt_s.at[i], xt_r.at[i], peer)

        def yt_copy(i):
            return remote(ys.at[pl.ds(i * TILE_T, TILE_T)], yr.at[pl.ds(i * TILE_T, TILE_T)],
                          yt_s.at[i], yt_r.at[i], peer)

        def drain(srcs):
            def fn(k, fc):
                for cs in (y_copies(k, fc, srcs), x_copies(k, fc), s_copies(k, fc), f_copies(k, fc)):
                    for c in cs:
                        c.wait_send()

            @pl.loop(0, NCH)
            def _(k):
                sized(k, fn)

        def generator(p, xb, wub, wdb):
            w_start, w_wait = w_stream(wub, wdb)
            for k in range(NCH):
                for c in y_copies(k, SMALL if k < N_SMALL else LARGE, gen_src):
                    c.start()
            for i in range(NTT):
                xt_copy(i).start()

            def x_load(t, slot):
                return local(x.at[pl.ds(pl.multiple_of(t * TILE, TILE), TILE)], xb.at[slot], lx.at[slot])

            def p_out(t):
                d = pl.ds(pl.multiple_of(t * TILE, TILE), TILE)
                return local(p.at[d], pout.at[d], lp.at[t])

            x_load(0, 0).start()

            @pl.loop(0, n_tok_g // 256)
            def _(i):
                p[pl.ds(pl.multiple_of(i * 256, 256), 256)] = jnp.zeros((256, D), F32)

            A, Bs = step_a(gen_src), step_b(gen_src)
            for k in range(2):
                sized(k, A)
                sized(k, Bs)
                sized(k, step_c)
            sized(0, step_d)
            arrive(0, SMALL)
            w_start(0, SMALL, 0)
            sized(2, A)

            def tile_math(t, xs, s, fc):
                h = TILE // 2
                base = pl.multiple_of(t * TILE, TILE)
                if fc == LARGE:
                    g = fc // 2
                    pre_a = dot(xb[xs], wub[s, :, :g])
                    u_a = gelu_bf16(pre_a)
                    pre_b = dot(xb[xs], wub[s, :, g:])
                    u = jnp.concatenate([u_a, gelu_bf16(pre_b)], axis=1)
                    p[pl.ds(base, TILE)] += dot(u, wdb[s])
                    return
                pre_a = dot(xb[xs, :h], wub[s, :, :fc])
                u_a = gelu_bf16(pre_a)
                pre_b = dot(xb[xs, h:], wub[s, :, :fc])
                p[pl.ds(base, h)] += dot(u_a, wdb[s, :fc, :])
                u_b = gelu_bf16(pre_b)
                p[pl.ds(base + h, h)] += dot(u_b, wdb[s, :fc, :])

            def chunk(c, fc, sized):
                s = lax.rem(c, 2)
                w_wait(c, fc, s)

                def load_next(k, fck):
                    arrive(k, fck)

                    @pl.when(k < N_FIRST)
                    def _():
                        w_start(k, fck, 1 - s)

                @pl.loop(0, (NT + 1) // 2)
                def _(g):
                    @pl.when(g == 0)
                    def _():
                        sized(c + 2, Bs)

                    @pl.when(g == 1)
                    def _():
                        sized(c + 2, step_c)

                    @pl.when(g == 2)
                    def _():
                        sized(c + 1, step_d)

                    @pl.when(g == 3)
                    def _():
                        sized(c + 1, load_next)

                        @pl.when(c + 3 < NCH)
                        def _():
                            sized(c + 3, A)

                    @pl.loop(2 * g, jnp.minimum(2 * g + 2, NT))
                    def _(t):
                        xs = lax.rem(c * NT + t, 2)
                        x_load(t, xs).wait()
                        x_load(lax.rem(t + 1, NT), 1 - xs).start()
                        tile_math(t, xs, s, fc)

                    @pl.when(c == N_FIRST - 1)
                    def _():
                        @pl.loop(2 * g, jnp.minimum(2 * g + 2, NT))
                        def _(t):
                            p_out(t).start()

            @pl.loop(0, N_SMALL)
            def _(c):
                chunk(c, SMALL, sized)

            @pl.loop(N_SMALL, N_FIRST)
            def _(c):
                chunk(c, LARGE, lambda k, fn: fn(k, LARGE))

            for k in range(N_FIRST + 1, NCH):
                sized(k, step_d)
            x_load(0, (N_FIRST * NT) % 2).wait()
            for i in range(NTT):
                xt_copy(i).wait_send()
            drain(gen_src)
            for k in range(N_FIRST + 1, NCH):
                sized(k, arrive)
            for t in range(NT):
                p_out(t).wait()
            for i in range(NTT):
                yt_copy(i).wait_recv()

        def trainer(p, st, xb, wub, wdb):
            w_start, w_wait = w_stream(wub, wdb)
            rate = lr[0]

            def u_load(k, fc):
                f = pl.ds(piece_off(k, fc), fc)
                return (local(w_up.at[:, f], st.at[pl.ds(0, S), pl.ds(0, fc)], l0.at[0]),
                        local(g_up.at[:, f], st.at[pl.ds(S, S), pl.ds(0, fc)], l0.at[1]),
                        local(w_dn.at[f, :], st.at[pl.ds(2 * S, fc), pl.ds(0, S)], l0.at[2]),
                        local(g_dn.at[f, :], st.at[pl.ds(2 * S + LARGE, fc), pl.ds(0, S)], l0.at[3]))

            def u_store(k, fc):
                f = pl.ds(piece_off(k, fc), fc)
                return (local(wub.at[0, pl.ds(0, S), pl.ds(0, fc)], pay_up.at[:, f], l0.at[4]),
                        local(wdb.at[0, pl.ds(0, fc), pl.ds(0, S)], pay_dn.at[f, :], l0.at[5]))

            def u_start(k, fc):
                for c in u_load(k, fc):
                    c.start()

            def u_math(k, fc):
                for c in u_load(k, fc):
                    c.wait()
                w = st[:S, :fc]
                new = w - rate * st[S:2 * S, :fc]
                wub[0, :S, :fc] = (new - w).astype(BF)
                w = st[2 * S:2 * S + fc, :S]
                new = w - rate * st[2 * S + LARGE:2 * S + LARGE + fc, :S]
                wdb[0, :fc, :S] = (new - w).astype(BF)
                for c in u_store(k, fc):
                    c.start()

            def u_send(k, fc):
                for c in u_store(k, fc):
                    c.wait()
                for c in y_copies(k, fc, trn_src):
                    c.start()

            for k in range(LEAD_T):
                sized(k, u_start)
                sized(k, u_math)
                sized(k, u_send)
            A, Bs = step_a(trn_src), step_b(trn_src)

            @pl.loop(0, NCH)
            def _(k):
                sized(k + LEAD_T, u_start)
                sized(k, A)
                sized(k + LEAD_T, u_math)
                sized(k, Bs)
                sized(k + LEAD_T, u_send)
                sized(k, step_c)
                sized(k - 1, step_d)

            def x_load(i):
                return local(xr.at[pl.ds(i * TILE_T, TILE_T)], xb.at[0], lx.at[0])

            def y_out(i):
                return local(xb.at[1], ys.at[pl.ds(i * TILE_T, TILE_T)], lx.at[1])

            for k in range(DEPTH - 1):
                arrive(k, SMALL)
                w_start(k, SMALL, k)

            @pl.loop(0, NTT)
            def _(i):
                xt_copy(i).wait_recv()
                x_load(i).start()
                p[...] = jnp.zeros((TILE_T, D), F32)
                x_load(i).wait()

                def piece(k, fc):
                    s = lax.rem(i * NCH + k, DEPTH)
                    w_wait(k, fc, s)
                    ahead = lax.rem(i * NCH + k + DEPTH - 1, DEPTH)

                    def nxt(kn, fcn):
                        @pl.when(i == 0)
                        def _():
                            arrive(kn, fcn)
                        w_start(kn, fcn, ahead)
                    if fc == LARGE:
                        @pl.when(jnp.logical_and(k == NCH - 6, i == 0))
                        def _():
                            step_d(NCH - 1, LARGE)
                    sized(k + DEPTH - 1, nxt)

                    @pl.when(jnp.logical_and(k + DEPTH - 1 >= NCH, i < NTT - 1))
                    def _():
                        w_start(k + DEPTH - 1 - NCH, SMALL, ahead)

                    trainer_math(p, xb, wub, wdb, s, fc)

                @pl.loop(0, N_SMALL)
                def _(k):
                    piece(k, SMALL)

                @pl.loop(N_SMALL, NCH)
                def _(k):
                    piece(k, LARGE)

                xb[1] = (xb[0].astype(F32) + p[...]).astype(BF)
                y_out(i).start()
                y_out(i).wait()
                yt_copy(i).start()

            drain(trn_src)
            for i in range(NTT):
                yt_copy(i).wait_send()

        @pl.when(is_gen)
        def _():
            pl.run_scoped(generator, pltpu.VMEM((n_tok_g, D), F32), pltpu.VMEM((2, TILE, D), BF),
                          pltpu.VMEM((2, D, LARGE), BF), pltpu.VMEM((2, LARGE, D), BF))

        @pl.when(jnp.logical_not(is_gen))
        def _():
            pl.run_scoped(trainer, pltpu.VMEM((TILE_T, D), F32), pltpu.VMEM((2 * S + 2 * LARGE, LARGE), F32),
                          pltpu.VMEM((2, TILE_T, D), BF),
                          pltpu.VMEM((DEPTH, D, LARGE), BF), pltpu.VMEM((DEPTH, LARGE, D), BF))

    def trainer_math(p, xb, wub, wdb, s, fc):
        h = TILE_T // 2
        pre_a = dot(xb[0, :h], wub[s, :, :fc])
        u_a = gelu_bf16(pre_a)
        pre_b = dot(xb[0, h:], wub[s, :, :fc])
        p[:h] += dot(u_a, wdb[s, :fc, :])
        u_b = gelu_bf16(pre_b)
        p[h:] += dot(u_b, wdb[s, :fc, :])

    def first(lr, w_up, w_dn, g_up, g_dn, old_up, old_dn, x):
        sds = jax.ShapeDtypeStruct
        outs = (sds((S, F), BF), sds((F, S), BF), sds((S, F), BF), sds((F, S), BF),
                sds((D, F), BF), sds((F, D), BF),
                sds((n_tok_t, D), BF), sds((n_tok_t, D), BF), sds((n_tok_t, D), BF),
                sds((n_tok_g, D), F32))
        dma = pltpu.SemaphoreType.DMA
        anyspace = pl.BlockSpec(memory_space=pl.ANY)
        return pl.pallas_call(
            kern,
            out_shape=outs,
            in_specs=[pl.BlockSpec(memory_space=pltpu.SMEM)] + [anyspace] * 7,
            out_specs=[anyspace] * len(outs),
            scratch_shapes=[
                pltpu.VMEM((S, LARGE), BF), pltpu.VMEM((LARGE, S), BF),
                pltpu.VMEM((S, LARGE), BF), pltpu.VMEM((LARGE, S), BF),
            ] + [dma((NCH, 2))] * 8 + [dma((NTT,))] * 4 + [
                dma((4,)), dma((2,)), dma((DEPTH, 2)), dma((2,)), dma((NT,)), dma((6,)),
            ],
            compiler_params=pltpu.CompilerParams(
                collective_id=0, has_side_effects=True, vmem_limit_bytes=VMEM_BYTES),
            name="sync_and_mlp",
        )(lr, w_up, w_dn, g_up, g_dn, old_up, old_dn, x)

    bu, bd = S // (NT + 1), F // (NT + 1)

    def kern2(role, lr, x_ref, p_ref, wu_ref, wd_ref, yr_ref, w_up, g_up, w_dn, g_dn,
              y_ref, new_up, new_dn, uw, ug, dw, dg, sem):
        t = pl.program_id(0)
        is_gen = lax.axis_index("side") == 1

        def in_copies():
            u, d = pl.ds(t * bu, bu), pl.ds(t * bd, bd)
            return (pltpu.make_async_copy(w_up.at[u], uw, sem.at[0]),
                    pltpu.make_async_copy(g_up.at[u], ug, sem.at[1]),
                    pltpu.make_async_copy(w_dn.at[d], dw, sem.at[2]),
                    pltpu.make_async_copy(g_dn.at[d], dg, sem.at[3]))

        def out_copies():
            u, d = pl.ds(t * bu, bu), pl.ds(t * bd, bd)
            return (pltpu.make_async_copy(uw, new_up.at[u], sem.at[4]),
                    pltpu.make_async_copy(dw, new_dn.at[d], sem.at[5]))

        @pl.when(jnp.logical_not(is_gen))
        def _():
            for c in in_copies():
                c.start()
            y_ref[...] = jnp.zeros_like(y_ref)
            for c in in_copies():
                c.wait()
            uw[...] = uw[...] - lr[0] * ug[...]
            dw[...] = dw[...] - lr[0] * dg[...]
            for c in out_copies():
                c.start()
            for c in out_copies():
                c.wait()

        @pl.when(is_gen)
        def _():
            @pl.when(t == 0)
            def _():
                uw[...] = jnp.zeros_like(uw)
                dw[...] = jnp.zeros_like(dw)

            for c in out_copies():
                c.start()

        @pl.when(is_gen & (t == NT))
        def _():
            y_ref[...] = yr_ref[...]

        @pl.when(is_gen & (t < NT))
        def _():
            h = TILE // 2
            pre_a = dot(x_ref[:h], wu_ref[...])
            u_a = gelu_bf16(pre_a)
            pre_b = dot(x_ref[h:], wu_ref[...])
            y_ref[:h] = (x_ref[:h].astype(F32) + (p_ref[:h] + dot(u_a, wd_ref[...]))).astype(BF)
            u_b = gelu_bf16(pre_b)
            y_ref[h:] = (x_ref[h:].astype(F32) + (p_ref[h:] + dot(u_b, wd_ref[...]))).astype(BF)

        @pl.when(is_gen)
        def _():
            for c in out_copies():
                c.wait()

    def second(role, lr, x, pout, wg_up, wg_dn, yr, w_up, g_up, w_dn, g_dn):
        fs = N_SECOND * LARGE
        assert bu * (NT + 1) == S and bd * (NT + 1) == F and bu % 8 == 0 and bd % 8 == 0
        once = pl.Buffered(1)
        anyspace = pl.BlockSpec(memory_space=pl.ANY)
        return pl.pallas_call(
            kern2,
            out_shape=(jax.ShapeDtypeStruct((B, D), BF),
                       jax.ShapeDtypeStruct((S, F), F32), jax.ShapeDtypeStruct((F, S), F32)),
            grid_spec=pltpu.PrefetchScalarGridSpec(
                num_scalar_prefetch=1,
                grid=(NT + 1,),
                in_specs=[
                    pl.BlockSpec(memory_space=pltpu.SMEM),
                    pl.BlockSpec((TILE, D), lambda t, role: (jnp.minimum(t, NT - 1) * role[0], 0)),
                    pl.BlockSpec((TILE, D), lambda t, role: (jnp.minimum(t, NT - 1) * role[0], 0)),
                    pl.BlockSpec((D, fs), lambda t, role: (0, 0), pipeline_mode=once),
                    pl.BlockSpec((fs, D), lambda t, role: (0, 0), pipeline_mode=once),
                    pl.BlockSpec((n_tok_t, D), lambda t, role: (0, 0), pipeline_mode=once),
                ] + [anyspace] * 4,
                out_specs=[pl.BlockSpec((TILE, D), lambda t, role: (t, 0)), anyspace, anyspace],
                scratch_shapes=[
                    pltpu.VMEM((bu, F), F32), pltpu.VMEM((bu, F), F32),
                    pltpu.VMEM((bd, S), F32), pltpu.VMEM((bd, S), F32),
                    pltpu.SemaphoreType.DMA((6,)),
                ],
            ),
            compiler_params=pltpu.CompilerParams(vmem_limit_bytes=VMEM_BYTES),
            name="last_pieces",
        )(role, lr, x, pout, wg_up, wg_dn, yr, w_up, g_up, w_dn, g_dn)

    return first, second


def solution(mesh):
    reps = mesh.shape["rep"]
    up_spec = P("side", None, "rep", None)
    down_spec = P("side", None, None, "rep")
    copy_spec = P("side", "rep", None, None, None)
    token_spec = P("side", "rep", None, None)

    def local_step(w_up, w_down, g_up, g_down, learn_rate, old_up, old_down, prompts):
        B, D = prompts.shape[2:]
        F = w_up.shape[3]
        first, second = make_step(D, F, B, reps)
        x = prompts[0, 0]
        outs = first(learn_rate, w_up[0, 0], w_down[0, 0], g_up[0, 0], g_down[0, 0],
                     old_up[0, 0, 0], old_down[0, 0, 0], x)
        wg_up, wg_dn, yr, pout = outs[4], outs[5], outs[8], outs[9]
        role = lax.axis_index("side").astype(jnp.int32)[None]
        y, new_up, new_down = second(role, learn_rate, x, pout, wg_up, wg_dn, yr,
                                     w_up[0, 0], g_up[0, 0], w_down[0, 0], g_down[0, 0])
        return new_up[None, None], new_down[None, None], y[None, None]

    return jax.shard_map(
        local_step,
        mesh=mesh,
        in_specs=(up_spec, down_spec, up_spec, down_spec, P(None), copy_spec, copy_spec, token_spec),
        out_specs=(up_spec, down_spec, token_spec),
        check_vma=False,
    )
```
